512 devices in a mesh: vocab: 64 (over z, y), pipe: 8 (over x, core).
Axes of the slice: x: 4, y: 8, z: 8, core: 2. Of those that a mesh axis runs over, the one named last changes fastest.
Arguments:
- hidden_a: bfloat16 [2048, 4096], P('pipe', 'vocab'), parts along dimension 0, may hold values from -8 to 8, as said below
- labels_a: int32 [2048], P('pipe'), parts along dimension 0, may hold values from 0 to 32767
- hidden_b: bfloat16 [2048, 4096], P('pipe', 'vocab'), parts along dimension 0, may hold values from -8 to 8, as said below
- labels_b: int32 [2048], P('pipe'), parts along dimension 0, may hold values from 0 to 32767
- loss_cotangent: float32 [2048], P('pipe'), parts along dimension 0, may hold values from -192 to 192
- out_weight: bfloat16 [32768, 32768], P('pipe', 'vocab'), parts along dimension 0, may hold values from -0.28125 to 0.28125, as said below
Outputs:
- logits_a: bfloat16 [2048, 32768], P('pipe', 'vocab'), parts along dimension 0
- loss_a: float32 [2048], P('pipe'), parts along dimension 0
- amax_scale: float32 [8], P('pipe'), parts along dimension 0
- grad_hidden_b: bfloat16 [2048, 4096], P('pipe', 'vocab'), parts along dimension 0
The draws below stay inside these ranges and needn't reach their ends.
There are 8 independent parts, one for each index of `pipe`. The reference program is written for one: setup_inputs(seed, part) draws one part's arguments, and reference() takes and returns one part's arrays. A program takes and returns all parts, laid end to end along the dimension named above; each array names one. Nothing has to cross between parts.
Inputs may be any that keep to these rules, and one draw needn't show every extreme that they name: `hidden_a`: hidden states of order one. `hidden_b`: hidden states of order one. `out_weight`: entries of scale 3 over the square root of 4096.
All inputs are finite; a program needn't handle non-finite values. Where the reference program divides by a largest or mean magnitude, that divisor is 1e-20 or more.
Results may differ from the reference program's by a relative error of at most 0.0048.
Values may be sent and summed in bfloat16 or wider, within the bound.
No kernel may reach another device: no remote copies, remote signals or barrier semaphores. Data moves between devices by JAX's collectives and lax.ppermute only.
A program may use at most 64 MiB of HBM per device.

```python
import jax
import jax.numpy as jnp
from jax import lax

D = 4096
TOK_A = 256
TOK_B = 256
VOCAB = 32768


def weight_matrix(key):
    raw = jax.random.normal(jax.random.fold_in(key, 11), (D, VOCAB), jnp.float32)
    return jnp.clip(raw, -6.0, 6.0) * (3.0 / D ** 0.5)


def hidden_rows(key, count, salt):
    base = jax.random.normal(jax.random.fold_in(key, salt), (count, D), jnp.float32)
    return jnp.clip(base, -8.0, 8.0)


def draw_out_weight(key, part):
    return weight_matrix(key).astype(jnp.bfloat16)


def draw_hidden_a(key, part):
    return hidden_rows(key, TOK_A, 101).astype(jnp.bfloat16)


def draw_hidden_b(key, part):
    return hidden_rows(key, TOK_B, 211).astype(jnp.bfloat16)


def with_ends(values, key, smallest, largest):
    place = [jax.random.randint(jax.random.fold_in(key, axis), (), 0, length) for axis, length in enumerate(values.shape)]
    widest = values.shape.index(max(values.shape))
    next_to = place[:widest] + [(place[widest] + 1) % values.shape[widest]] + place[widest + 1:]
    return values.at[tuple(place)].set(smallest).at[tuple(next_to)].set(largest)


def bell_draw(own_key, extent, deviation, bound, held_as=jnp.bfloat16):
    drawn = jax.random.normal(own_key, extent, jnp.float32) * deviation
    return jnp.minimum(jnp.maximum(drawn, -bound), bound).astype(held_as)


def setup_inputs(seed: int = 0, part: int = 0) -> dict:
    arg_keys = jax.random.split(jax.random.key(seed), 7)
    part_splits = jax.random.split(jax.random.fold_in(arg_keys[6], part), 7)
    hidden_a = draw_hidden_a(jax.random.fold_in(jax.random.fold_in(arg_keys[6], part), 71), part)
    labels_a = with_ends(jax.random.randint(part_splits[1], (TOK_A,), 0, VOCAB), jax.random.fold_in(part_splits[1], 1), 0, VOCAB - 1).astype(jnp.int32)
    hidden_b = draw_hidden_b(jax.random.fold_in(jax.random.fold_in(arg_keys[6], part), 71), part)
    labels_b = with_ends(jax.random.randint(part_splits[3], (TOK_B,), 0, VOCAB), jax.random.fold_in(part_splits[3], 1), 0, VOCAB - 1).astype(jnp.int32)
    loss_cotangent = bell_draw(part_splits[4], (TOK_B,), 32.0, 192.0, jnp.float32)
    out_weight = draw_out_weight(jax.random.fold_in(jax.random.fold_in(arg_keys[6], part), 71), part)
    return dict(hidden_a=hidden_a, labels_a=labels_a, hidden_b=hidden_b, labels_b=labels_b, loss_cotangent=loss_cotangent, out_weight=out_weight)


def reference(hidden_a, labels_a, hidden_b, labels_b, loss_cotangent, out_weight):
    scores_a = jnp.dot(hidden_a, out_weight, preferred_element_type=jnp.float32)
    logits_a = scores_a.astype(jnp.bfloat16)
    peak_a = jnp.max(scores_a, axis=1)
    total_a = jnp.sum(jnp.exp(scores_a - peak_a[:, None]), axis=1)
    label_a = jnp.take_along_axis(scores_a, labels_a.astype(jnp.int32)[:, None], axis=1)[:, 0]
    loss_a = jnp.log(total_a) + peak_a - label_a
    amax_scale = (448.0 / jnp.max(jnp.abs(scores_a))).reshape(1).astype(jnp.float32)
    scores_b = jnp.dot(hidden_b, out_weight, preferred_element_type=jnp.float32)
    peak_b = jnp.max(scores_b, axis=1)
    total_b = jnp.sum(jnp.exp(scores_b - peak_b[:, None]), axis=1)
    columns = lax.broadcasted_iota(jnp.int32, scores_b.shape, 1)
    onehot = (columns == labels_b.astype(jnp.int32)[:, None]).astype(jnp.float32)
    probs = jnp.exp(scores_b - peak_b[:, None]) / total_b[:, None]
    dlogits_b = ((probs - onehot) * loss_cotangent[:, None]).astype(jnp.bfloat16)
    grad_full = lax.dot_general(dlogits_b, out_weight, (((1,), (1,)), ((), ())), preferred_element_type=jnp.float32)
    return logits_a, loss_a, amax_scale, grad_full.astype(jnp.bfloat16)
```

```python
import jax
import jax.numpy as jnp
from jax import lax
from jax.sharding import Mesh
from jax.sharding import PartitionSpec as P


Z, Y = "vocab_0", "vocab_1"
VOCAB = (Z, Y)


def shifted(x, axis, by):
    n = lax.axis_size(axis)
    return lax.ppermute(x, axis, [(i, (i + by) % n) for i in range(n)])


def from_everyone(x, axis):
    devices = 1
    for name in axis if isinstance(axis, tuple) else (axis,):
        devices *= lax.axis_size(name)
    return lax.all_to_all(jnp.broadcast_to(x[None], (devices, *x.shape)), axis, 0, 0, tiled=True)


def ring_blocks(x, axis):
    n = lax.axis_size(axis)
    yield 0, x
    ahead = behind = x
    for step in range(1, n // 2 + 1):
        behind = shifted(behind, axis, 1)
        yield -step, behind
        if 2 * step < n:
            ahead = shifted(ahead, axis, -1)
            yield step, ahead


def ring_sum(term, axis):
    n = lax.axis_size(axis)
    left = right = None
    for far in range(n // 2, 0, -1):
        own = term(-far)
        left = own if left is None else left.astype(jnp.float32) + own
        left = shifted(left.astype(jnp.bfloat16), axis, -1)
        if 2 * far < n:
            own = term(far)
            right = own if right is None else right.astype(jnp.float32) + own
            right = shifted(right.astype(jnp.bfloat16), axis, 1)
    return term(0) + left.astype(jnp.float32) + right.astype(jnp.float32)


def shards(hidden_a, labels_a, hidden_b, labels_b, loss_cotangent, out_weight):
    tokens = hidden_a.shape[0]
    depth, columns = out_weight.shape
    nz, ny = lax.axis_size(Z), lax.axis_size(Y)
    rows = depth // nz
    z = lax.axis_index(Z)
    offset = lax.axis_index(VOCAB) * columns

    def weight_rows(step):
        return lax.dynamic_slice_in_dim(out_weight, (z + step + nz) % nz * rows, rows, 0)

    own = jnp.concatenate([hidden_b.T, hidden_a.T], axis=1)
    mine = from_everyone(own, Y).reshape(rows, 2 * tokens)

    def scores_of(block):
        total = None
        for step, part in ring_blocks(block, Z):
            term = lax.dot_general(
                part, weight_rows(step), (((0,), (0,)), ((), ())), preferred_element_type=jnp.float32
            )
            total = term if total is None else total + term
        return total

    scores_b = scores_of(mine[:, :tokens])
    scores_a = scores_of(mine[:, tokens:])
    column = offset + lax.broadcasted_iota(jnp.int32, (1, columns), 1)

    def log_total(scores):
        peak = jnp.max(scores, axis=1)
        return peak + jnp.log(jnp.sum(jnp.exp(scores - peak[:, None]), axis=1))

    label_own = jnp.sum(jnp.where(column == labels_a[:, None], scores_a, 0.0), axis=1)
    largest = jnp.full((128,), jnp.max(jnp.abs(scores_a)))
    line = jnp.concatenate([log_total(scores_b), log_total(scores_a), label_own, largest])
    lines = from_everyone(line.reshape(1, -1), VOCAB).reshape(-1, line.size)

    def joined(logs):
        peak = jnp.max(logs, axis=0)
        return peak + jnp.log(jnp.sum(jnp.exp(logs - peak), axis=0))

    log_b = joined(lines[:, :tokens])
    log_a = joined(lines[:, tokens : 2 * tokens])
    label_a = jnp.sum(lines[:, 2 * tokens : 3 * tokens], axis=0)
    loss_a = log_a - label_a
    amax_scale = (448.0 / jnp.max(lines[:, 3 * tokens :])).reshape(1).astype(jnp.float32)

    onehot = (column == labels_b[:, None]).astype(jnp.float32)
    dlogits_b = ((jnp.exp(scores_b - log_b[:, None]) - onehot) * loss_cotangent[:, None]).astype(
        jnp.bfloat16
    )
    grad_terms = lax.dot_general(
        out_weight, dlogits_b, (((1,), (1,)), ((), ())), preferred_element_type=jnp.float32
    )

    def grad_rows(step):
        return lax.dynamic_slice_in_dim(grad_terms, (z + step + nz) % nz * rows, rows, 0)

    summed = ring_sum(grad_rows, Z).astype(jnp.bfloat16).reshape(ny, rows // ny, tokens)
    parts = lax.all_to_all(summed, Y, 0, 0, tiled=True)
    grad_hidden_b = jnp.sum(parts.astype(jnp.float32), axis=0).astype(jnp.bfloat16).T
    return (scores_a.astype(jnp.bfloat16), loss_a, amax_scale, grad_hidden_b)


def solution(mesh):
    finer = Mesh(mesh.devices.reshape(8, 8, mesh.shape["pipe"]), (Z, Y, "pipe"))
    placed = (P("pipe", VOCAB), P("pipe"), P("pipe", VOCAB), P("pipe"), P("pipe"), P("pipe", VOCAB))
    return jax.shard_map(
        shards,
        mesh=finer,
        in_specs=placed,
        out_specs=(P("pipe", VOCAB), P("pipe"), P("pipe"), P("pipe", VOCAB)),
        check_vma=False,
    )
```

```python
import jax
import jax.numpy as jnp
from jax import lax
from jax.sharding import Mesh
from jax.sharding import PartitionSpec as P


Z, Y = "vocab_0", "vocab_1"
VOCAB = (Z, Y)


def shifted(x, axis, by):
    n = lax.axis_size(axis)
    return lax.ppermute(x, axis, [(i, (i + by) % n) for i in range(n)])


def from_everyone(x, axis):
    devices = 1
    for name in axis if isinstance(axis, tuple) else (axis,):
        devices *= lax.axis_size(name)
    return lax.all_to_all(jnp.broadcast_to(x[None], (devices, *x.shape)), axis, 0, 0, tiled=True)


def ring_blocks(x, axis):
    n = lax.axis_size(axis)
    yield 0, x
    ahead = behind = x
    for step in range(1, n // 2 + 1):
        behind = shifted(behind, axis, 1)
        yield -step, behind
        if 2 * step < n:
            ahead = shifted(ahead, axis, -1)
            yield step, ahead


def beside(i, n):
    return (i + 1) % n if i % 2 else (i - 1) % n


def paired_blocks(x, axis):
    n = lax.axis_size(axis)
    me = lax.axis_index(axis)

    def across(v, side):
        return lax.ppermute(v, axis, [(i, side(i)) for i in range(n)])

    def far(v):
        return v + 1 - 2 * (v % 2)

    def out(v):
        return (v + 2 * (v % 2) - 1 + n) % n

    yield me, x
    other = across(x, lambda i: i ^ 1)
    yield far(me), other
    moving = jnp.concatenate([x, other], axis=0)
    for step in range(2, n // 2 + 1):
        moving = across(moving, (lambda i: i ^ 1) if step % 2 else (lambda i: beside(i, n)))
        half = moving.shape[0] // 2
        first = me
        for back in range(step, 1, -1):
            first = far(first) if back % 2 else out(first)
        yield first, moving[:half]
        yield far(first), moving[half:]


def shards(hidden_a, labels_a, hidden_b, labels_b, loss_cotangent, out_weight):
    tokens = hidden_a.shape[0]
    depth, columns = out_weight.shape
    nz, ny = lax.axis_size(Z), lax.axis_size(Y)
    rows = depth // nz
    z = lax.axis_index(Z)
    offset = lax.axis_index(VOCAB) * columns

    def weight_rows(at):
        return lax.dynamic_slice_in_dim(out_weight, at * rows, rows, 0)

    own = jnp.concatenate([hidden_b.T, hidden_a.T], axis=1)
    mine = from_everyone(own, Y).reshape(rows, 2 * tokens)

    def scores_of(blocks):
        total = None
        for at, part in blocks:
            term = lax.dot_general(
                part, weight_rows(at), (((0,), (0,)), ((), ())), preferred_element_type=jnp.float32
            )
            total = term if total is None else total + term
        return total

    ring = (((z + step + nz) % nz, part) for step, part in ring_blocks(mine[:, :tokens], Z))
    scores_b = scores_of(ring)
    scores_a = scores_of(paired_blocks(mine[:, tokens:], Z))
    column = offset + lax.broadcasted_iota(jnp.int32, (1, columns), 1)

    def log_total(scores):
        peak = jnp.max(scores, axis=1)
        return peak + jnp.log(jnp.sum(jnp.exp(scores - peak[:, None]), axis=1))

    label_own = jnp.sum(jnp.where(column == labels_a[:, None], scores_a, 0.0), axis=1)
    largest = jnp.full((128,), jnp.max(jnp.abs(scores_a)))
    line = jnp.concatenate([log_total(scores_b), log_total(scores_a), label_own, largest])
    lines = from_everyone(line.reshape(1, -1), VOCAB).reshape(-1, line.size)

    def joined(logs):
        peak = jnp.max(logs, axis=0)
        return peak + jnp.log(jnp.sum(jnp.exp(logs - peak), axis=0))

    log_b = joined(lines[:, :tokens])
    log_a = joined(lines[:, tokens : 2 * tokens])
    label_a = jnp.sum(lines[:, 2 * tokens : 3 * tokens], axis=0)
    loss_a = log_a - label_a
    amax_scale = (448.0 / jnp.max(lines[:, 3 * tokens :])).reshape(1).astype(jnp.float32)

    onehot = (column == labels_b[:, None]).astype(jnp.float32)
    dlogits_b = ((jnp.exp(scores_b - log_b[:, None]) - onehot) * loss_cotangent[:, None]).astype(
        jnp.bfloat16
    )
    grad_terms = lax.dot_general(
        out_weight, dlogits_b, (((1,), (1,)), ((), ())), preferred_element_type=jnp.float32
    )

    partial = grad_terms.astype(jnp.bfloat16).reshape(nz * ny, rows // ny, tokens)
    parts = lax.all_to_all(partial, VOCAB, 0, 0, tiled=True)
    grad_hidden_b = jnp.sum(parts.astype(jnp.float32), axis=0).astype(jnp.bfloat16).T
    return (scores_a.astype(jnp.bfloat16), loss_a, amax_scale, grad_hidden_b)


def solution(mesh):
    finer = Mesh(mesh.devices.reshape(8, 8, mesh.shape["pipe"]), (Z, Y, "pipe"))
    placed = (P("pipe", VOCAB), P("pipe"), P("pipe", VOCAB), P("pipe"), P("pipe"), P("pipe", VOCAB))

    return jax.shard_map(
        shards,
        mesh=finer,
        in_specs=placed,
        out_specs=(P("pipe", VOCAB), P("pipe"), P("pipe"), P("pipe", VOCAB)),
        check_vma=False,
    )
```

```python
import jax
import jax.numpy as jnp
from jax import lax
from jax.sharding import Mesh
from jax.sharding import PartitionSpec as P


Z, Y = ("z_two", "z_one"), ("y_two", "y_one")
VOCAB = (*Z, *Y)
LATTICE = ("z_two", "y_two")
FLIPS = ((1, 0), (0, 1), (1, 1))


def size(axes):
    return lax.axis_size(axes)


def from_everyone(x, axes):
    return lax.all_to_all(jnp.broadcast_to(x[None], (size(axes), *x.shape)), axes, 0, 0, tiled=True)


def neighbour(i, n, shift):
    return (i + 1 - 2 * ((i + shift) % 2) + n) % n


def exchanged(x, flip, shift):
    nz, ny = size(Z), size(Y)
    pairs = []
    for z in range(nz):
        for y in range(ny):
            there = neighbour(z, nz, shift) if flip[0] else z, neighbour(y, ny, shift) if flip[1] else y
            pairs.append((z * ny + y, there[0] * ny + there[1]))
    return lax.ppermute(x, VOCAB, pairs)


def shards(hidden_a, labels_a, hidden_b, labels_b, loss_cotangent, out_weight):
    tokens, width = hidden_a.shape
    columns = out_weight.shape[1]
    offset = lax.axis_index(VOCAB) * columns
    lattice = size(LATTICE)
    half = lattice * width // 2
    by_class = out_weight.reshape(size(Z[0]), 2, size(Y[0]), 2, width, columns)

    def weight_rows(flip):
        z, y = lax.axis_index(Z[1]), lax.axis_index(Y[1])
        rows = lax.dynamic_index_in_dim(by_class, z + flip[0] - 2 * z * flip[0], 1, False)
        rows = lax.dynamic_index_in_dim(rows, y + flip[1] - 2 * y * flip[1], 2, False)
        return rows.reshape(2 * half, columns)

    weights = {flip: weight_rows(flip) for flip in ((0, 0), *FLIPS)}

    def product(block, rows):
        return lax.dot_general(
            block, rows, (((0,), (0,)), ((), ())), preferred_element_type=jnp.float32
        )

    own = jnp.concatenate([hidden_b.T, hidden_a.T], axis=1)
    mine = from_everyone(own, LATTICE).reshape(2 * half, 2 * tokens)
    scores = product(mine, weights[0, 0])
    for flip in FLIPS:
        for shift in range(2):
            at = slice(shift * half, (shift + 1) * half)
            with jax.named_scope(f"gather{flip[0]}{flip[1]}{shift}"):
                block = exchanged(mine[at], flip, shift)
            scores = scores + product(block, weights[flip][at])
    scores_b, scores_a = scores[:tokens], scores[tokens:]
    column = offset + lax.broadcasted_iota(jnp.int32, (1, columns), 1)

    def log_total(scores):
        peak = jnp.max(scores, axis=1)
        return peak + jnp.log(jnp.sum(jnp.exp(scores - peak[:, None]), axis=1))

    label_own = jnp.sum(jnp.where(column == labels_a[:, None], scores_a, 0.0), axis=1)
    largest = jnp.full((128,), jnp.max(jnp.abs(scores_a)))
    line = jnp.concatenate([log_total(scores_b), log_total(scores_a), label_own, largest])
    lines = from_everyone(line.reshape(1, -1), VOCAB).reshape(-1, line.size)

    def joined(logs):
        peak = jnp.max(logs, axis=0)
        return peak + jnp.log(jnp.sum(jnp.exp(logs - peak), axis=0))

    log_b = joined(lines[:, :tokens])
    log_a = joined(lines[:, tokens : 2 * tokens])
    label_a = jnp.sum(lines[:, 2 * tokens : 3 * tokens], axis=0)
    loss_a = log_a - label_a
    amax_scale = (448.0 / jnp.max(lines[:, 3 * tokens :])).reshape(1).astype(jnp.float32)

    onehot = (column == labels_b[:, None]).astype(jnp.float32)
    dlogits_b = ((jnp.exp(scores_b - log_b[:, None]) - onehot) * loss_cotangent[:, None]).astype(
        jnp.bfloat16
    )

    def grad_rows(flip):
        return lax.dot_general(
            weights[flip], dlogits_b, (((1,), (1,)), ((), ())), preferred_element_type=jnp.float32
        )

    terms = {flip: grad_rows(flip) for flip in ((0, 0), *FLIPS)}
    sums = []
    for shift in range(2):
        at = slice(shift * half, (shift + 1) * half)
        total = terms[0, 0][at]
        for flip in FLIPS:
            with jax.named_scope(f"scatter{flip[0]}{flip[1]}{shift}"):
                total = total + exchanged(terms[flip][at].astype(jnp.bfloat16), flip, shift).astype(
                    jnp.float32
                )
        sums.append(total.astype(jnp.bfloat16).reshape(lattice // 2, width, tokens))
    parts = lax.all_to_all(jnp.concatenate(sums), LATTICE, 0, 0, tiled=True)
    grad_hidden_b = jnp.sum(parts.astype(jnp.float32), axis=0).astype(jnp.bfloat16).T
    return (scores_a.astype(jnp.bfloat16), loss_a, amax_scale, grad_hidden_b)


def solution(mesh):
    finer = Mesh(mesh.devices.reshape(4, 2, 4, 2, mesh.shape["pipe"]), (*VOCAB, "pipe"))
    placed = (P("pipe", VOCAB), P("pipe"), P("pipe", VOCAB), P("pipe"), P("pipe"), P("pipe", VOCAB))
    return jax.shard_map(
        shards,
        mesh=finer,
        in_specs=placed,
        out_specs=(P("pipe", VOCAB), P("pipe"), P("pipe"), P("pipe", VOCAB)),
        check_vma=False,
    )
```

```python
import jax
import jax.numpy as jnp
from jax import lax
from jax.sharding import Mesh
from jax.sharding import PartitionSpec as P


Z, Y = ("z_two", "z_one"), ("y_two", "y_one")
VOCAB = (*Z, *Y)
LATTICE = ("z_two", "y_two")
FLIPS = ((1, 0), (0, 1), (1, 1))


def size(axes):
    return lax.axis_size(axes)


def from_everyone(x, axes):
    return lax.all_to_all(jnp.broadcast_to(x[None], (size(axes), *x.shape)), axes, 0, 0, tiled=True)


def neighbour(i, n, shift):
    return (i + 1 - 2 * ((i + shift) % 2) + n) % n


def exchanged(x, flip, shift):
    nz, ny = size(Z), size(Y)
    pairs = []
    for z in range(nz):
        for y in range(ny):
            there = neighbour(z, nz, shift) if flip[0] else z, neighbour(y, ny, shift) if flip[1] else y
            pairs.append((z * ny + y, there[0] * ny + there[1]))
    return lax.ppermute(x, VOCAB, pairs)


def shards(hidden_a, labels_a, hidden_b, labels_b, loss_cotangent, out_weight):
    tokens, width = hidden_a.shape
    columns = out_weight.shape[1]
    offset = lax.axis_index(VOCAB) * columns
    lattice = size(LATTICE)
    half = lattice * width // 2
    by_class = out_weight.reshape(size(Z[0]), 2, size(Y[0]), 2, width, columns)

    def weight_rows(flip):
        z, y = lax.axis_index(Z[1]), lax.axis_index(Y[1])
        at = (0, z + flip[0] - 2 * z * flip[0], 0, y + flip[1] - 2 * y * flip[1], 0, 0)
        counts = (by_class.shape[0], 1, by_class.shape[2], 1, width, columns)
        return lax.dynamic_slice(by_class, at, counts).reshape(2 * half, columns)

    weights = {flip: weight_rows(flip) for flip in ((0, 0), *FLIPS)}

    def product(block, rows):
        return lax.dot_general(
            block, rows, (((0,), (0,)), ((), ())), preferred_element_type=jnp.float32
        )

    def class_rows(hidden):
        return from_everyone(hidden.T, LATTICE).reshape(2 * half, tokens)

    mine_b = class_rows(hidden_b)
    mine_a = class_rows(hidden_a)
    scores_b = product(mine_b, weights[0, 0])
    for flip in FLIPS:
        for shift in range(2):
            at = slice(shift * half, (shift + 1) * half)
            block = exchanged(mine_b[at], flip, shift)
            scores_b = scores_b + product(block, weights[flip][at])
    scores_a = product(mine_a, weights[0, 0])
    for flip in FLIPS:
        block = exchanged(mine_a, flip, 1)
        scores_a = scores_a + product(block, weights[flip])
    column = offset + lax.broadcasted_iota(jnp.int32, (1, columns), 1)
    column_a = lax.optimization_barrier(column)

    def log_total(scores):
        peak = jnp.max(scores, axis=1)
        return peak + jnp.log(jnp.sum(jnp.exp(scores - peak[:, None]), axis=1))

    def joined(logs):
        peak = jnp.max(logs, axis=0)
        return peak + jnp.log(jnp.sum(jnp.exp(logs - peak), axis=0))

    log_b = joined(from_everyone(log_total(scores_b).reshape(1, -1), VOCAB).reshape(-1, tokens))
    label_own = jnp.sum(jnp.where(column_a == labels_a[:, None], scores_a, 0.0), axis=1)
    largest = jnp.full((128,), jnp.max(jnp.abs(scores_a)))
    line = jnp.concatenate([log_total(scores_a), label_own, largest])
    lines = from_everyone(line.reshape(1, -1), VOCAB).reshape(-1, line.size)
    loss_a = joined(lines[:, :tokens]) - jnp.sum(lines[:, tokens : 2 * tokens], axis=0)
    amax_scale = (448.0 / jnp.max(lines[:, 2 * tokens :])).reshape(1).astype(jnp.float32)

    onehot = (column == labels_b[:, None]).astype(jnp.float32)
    dlogits_b = ((jnp.exp(scores_b - log_b[:, None]) - onehot) * loss_cotangent[:, None]).astype(
        jnp.bfloat16
    )

    dlogits_b = lax.optimization_barrier(dlogits_b)

    def grad_rows(flip):
        return lax.dot_general(
            weights[flip], dlogits_b, (((1,), (1,)), ((), ())), preferred_element_type=jnp.float32
        )

    total = grad_rows((0, 0))
    for flip in FLIPS:
        total = total + exchanged(grad_rows(flip).astype(jnp.bfloat16), flip, 0).astype(jnp.float32)
    parts = total.astype(jnp.bfloat16).reshape(lattice, width, tokens)
    parts = lax.all_to_all(parts, LATTICE, 0, 0, tiled=True)
    grad_hidden_b = jnp.sum(parts.astype(jnp.float32), axis=0).astype(jnp.bfloat16).T
    return (scores_a.astype(jnp.bfloat16), loss_a, amax_scale, grad_hidden_b)


def solution(mesh):
    finer = Mesh(mesh.devices.reshape(4, 2, 4, 2, mesh.shape["pipe"]), (*VOCAB, "pipe"))
    placed = (P("pipe", VOCAB), P("pipe"), P("pipe", VOCAB), P("pipe"), P("pipe"), P("pipe", VOCAB))

    return jax.shard_map(
        shards,
        mesh=finer,
        in_specs=placed,
        out_specs=(P("pipe", VOCAB), P("pipe"), P("pipe"), P("pipe", VOCAB)),
        check_vma=False,
    )
```

```python
import jax
import jax.numpy as jnp
from jax import lax
from jax.sharding import Mesh
from jax.sharding import PartitionSpec as P


Z, Y = ("z_two", "z_one"), ("y_two", "y_one")
VOCAB = (*Z, *Y)
LATTICE, QUAD = ("z_two", "y_two"), ("z_one", "y_one")
FLIPS = ((1, 0), (0, 1), (1, 1))


def size(axes):
    return lax.axis_size(axes)


def from_everyone(x, axes):
    return lax.all_to_all(jnp.broadcast_to(x[None], (size(axes), *x.shape)), axes, 0, 0, tiled=True)


def pieces(x):
    high = lax.reduce_precision(x, 8, 7)
    middle = lax.reduce_precision(x - high, 8, 7)
    return high, middle, x - high - middle


def neighbour(i, n, shift):
    return (i + 1 - 2 * ((i + shift) % 2) + n) % n


def exchanged(x, flip, shift):
    nz, ny = size(Z), size(Y)
    pairs = []
    for z in range(nz):
        for y in range(ny):
            there = neighbour(z, nz, shift) if flip[0] else z, neighbour(y, ny, shift) if flip[1] else y
            pairs.append((z * ny + y, there[0] * ny + there[1]))
    return lax.ppermute(x, VOCAB, pairs)


def shards(hidden_a, labels_a, hidden_b, labels_b, loss_cotangent, out_weight):
    tokens, width = hidden_a.shape
    columns = out_weight.shape[1]
    offset = lax.axis_index(VOCAB) * columns
    lattice = size(LATTICE)
    half = lattice * width // 2
    by_class = out_weight.reshape(size(Z[0]), 2, size(Y[0]), 2, width, columns)

    def weight_rows(flip):
        z, y = lax.axis_index(Z[1]), lax.axis_index(Y[1])
        at = (0, z + flip[0] - 2 * z * flip[0], 0, y + flip[1] - 2 * y * flip[1], 0, 0)
        counts = (by_class.shape[0], 1, by_class.shape[2], 1, width, columns)
        return lax.dynamic_slice(by_class, at, counts).reshape(2 * half, columns)

    weights = {flip: weight_rows(flip) for flip in ((0, 0), *FLIPS)}

    def product(block, rows):
        return lax.dot_general(
            block, rows, (((0,), (0,)), ((), ())), preferred_element_type=jnp.float32
        )

    def class_rows(hidden):
        return from_everyone(hidden.T, LATTICE).reshape(2 * half, tokens)

    mine_b = class_rows(hidden_b)
    mine_a = class_rows(hidden_a)

    def scores_of(mine, shift):
        scores = product(mine, weights[0, 0])
        for flip in FLIPS:
            block = exchanged(mine, flip, shift)
            scores = scores + product(block, weights[flip])
        return scores

    scores_b = scores_of(mine_b, 0)
    scores_a = scores_of(mine_a, 1)
    column = offset + lax.broadcasted_iota(jnp.int32, (1, columns), 1)
    column_a = lax.optimization_barrier(column)

    def log_total(scores):
        peak = jnp.max(scores, axis=1)
        return peak + jnp.log(jnp.sum(jnp.exp(scores - peak[:, None]), axis=1))

    def joined(logs):
        peak = jnp.max(logs, axis=0)
        return peak + jnp.log(jnp.sum(jnp.exp(logs - peak), axis=0))

    log_b = joined(from_everyone(log_total(scores_b).reshape(1, -1), VOCAB).reshape(-1, tokens))
    label_own = jnp.sum(jnp.where(column_a == labels_a[:, None], scores_a, 0.0), axis=1)
    largest = jnp.full((128,), jnp.max(jnp.abs(scores_a)))
    line = jnp.concatenate([log_total(scores_a), label_own, largest])
    quad = from_everyone(line.reshape(1, -1), QUAD).reshape(-1, line.size)
    log_a = pieces(joined(quad[:, :tokens]))
    label_a = pieces(jnp.sum(quad[:, tokens : 2 * tokens], axis=0))
    lane = lax.broadcasted_iota(jnp.int32, (tokens,), 0)
    high, middle, low = pieces(jnp.max(quad[:, 2 * tokens :]))
    largest = jnp.where(lane == 0, high, jnp.where(lane == 1, middle, low))
    riders = jnp.stack([*log_a, *label_a, largest, jnp.zeros_like(largest)]).astype(jnp.bfloat16)

    onehot = (column == labels_b[:, None]).astype(jnp.float32)
    dlogits_b = ((jnp.exp(scores_b - log_b[:, None]) - onehot) * loss_cotangent[:, None]).astype(
        jnp.bfloat16
    )

    dlogits_b = lax.optimization_barrier(dlogits_b)

    def grad_rows(flip):
        return lax.dot_general(
            weights[flip], dlogits_b, (((1,), (1,)), ((), ())), preferred_element_type=jnp.float32
        )

    total = lax.optimization_barrier(grad_rows((0, 0)))
    for flip in FLIPS:
        total = total + exchanged(grad_rows(flip).astype(jnp.bfloat16), flip, 0).astype(jnp.float32)
    parts = total.astype(jnp.bfloat16).reshape(lattice, width, tokens)
    parts = jnp.concatenate([parts, jnp.broadcast_to(riders[None], (lattice, *riders.shape))], axis=1)
    parts = lax.all_to_all(parts, LATTICE, 0, 0, tiled=True)
    grad_hidden_b = jnp.sum(parts[:, :width].astype(jnp.float32), axis=0).astype(jnp.bfloat16).T
    came = parts[:, width:].astype(jnp.float32)
    loss_a = joined(came[:, :3].sum(axis=1)) - came[:, 3:6].sum(axis=(0, 1))
    amax_scale = (448.0 / jnp.max(came[:, 6, :3].sum(axis=1))).reshape(1).astype(jnp.float32)
    return (scores_a.astype(jnp.bfloat16), loss_a, amax_scale, grad_hidden_b)


def solution(mesh):
    finer = Mesh(mesh.devices.reshape(4, 2, 4, 2, mesh.shape["pipe"]), (*VOCAB, "pipe"))
    placed = (P("pipe", VOCAB), P("pipe"), P("pipe", VOCAB), P("pipe"), P("pipe"), P("pipe", VOCAB))

    return jax.shard_map(
        shards,
        mesh=finer,
        in_specs=placed,
        out_specs=(P("pipe", VOCAB), P("pipe"), P("pipe"), P("pipe", VOCAB)),
        check_vma=False,
    )
```

```python
import jax
import jax.numpy as jnp
from jax import lax
from jax.sharding import Mesh
from jax.sharding import PartitionSpec as P


Z, Y = ("z_two", "z_one"), ("y_two", "y_one")
VOCAB = (*Z, *Y)
LATTICE = ("z_two", "y_two")
FLIPS = ((1, 1), (1, 0), (0, 1))


def size(axes):
    return lax.axis_size(axes)


def from_everyone(x, axes):
    return lax.all_to_all(jnp.broadcast_to(x[None], (size(axes), *x.shape)), axes, 0, 0, tiled=True)


def neighbour(i, n, shift):
    return (i + 1 - 2 * ((i + shift) % 2) + n) % n


def exchanged(x, flip):
    shift = flip[0] * flip[1]
    nz, ny = size(Z), size(Y)
    pairs = []
    for z in range(nz):
        for y in range(ny):
            there = neighbour(z, nz, shift) if flip[0] else z, neighbour(y, ny, shift) if flip[1] else y
            pairs.append((z * ny + y, there[0] * ny + there[1]))
    return lax.ppermute(x, VOCAB, pairs)


def shards(hidden_a, labels_a, hidden_b, labels_b, loss_cotangent, out_weight):
    tokens, width = hidden_a.shape
    columns = out_weight.shape[1]
    offset = lax.axis_index(VOCAB) * columns
    lattice = size(LATTICE)
    half = lattice * width // 2
    by_class = out_weight.reshape(size(Z[0]), 2, size(Y[0]), 2, width, columns)

    def weight_rows(flip):
        z, y = lax.axis_index(Z[1]), lax.axis_index(Y[1])
        at = (0, z + flip[0] - 2 * z * flip[0], 0, y + flip[1] - 2 * y * flip[1], 0, 0)
        counts = (by_class.shape[0], 1, by_class.shape[2], 1, width, columns)
        return lax.dynamic_slice(by_class, at, counts).reshape(2 * half, columns)

    weights = {flip: weight_rows(flip) for flip in ((0, 0), *FLIPS)}

    def product(block, rows):
        return lax.dot_general(
            block, rows, (((0,), (0,)), ((), ())), preferred_element_type=jnp.float32
        )

    own = jnp.concatenate([hidden_b.T, hidden_a.T], axis=1)
    mine = from_everyone(own, LATTICE).reshape(2 * half, 2 * tokens)
    scores = product(mine, weights[0, 0])
    for flip in FLIPS:
        block = exchanged(mine, flip)
        scores = scores + product(block, weights[flip])
    scores_b, scores_a = scores[:tokens], scores[tokens:]
    column = offset + lax.broadcasted_iota(jnp.int32, (1, columns), 1)

    def log_total(scores):
        peak = jnp.max(scores, axis=1)
        return peak + jnp.log(jnp.sum(jnp.exp(scores - peak[:, None]), axis=1))

    label_own = jnp.sum(jnp.where(column == labels_a[:, None], scores_a, 0.0), axis=1)
    largest = jnp.full((128,), jnp.max(jnp.abs(scores_a)))
    line = jnp.concatenate([log_total(scores_b), log_total(scores_a), label_own, largest])
    lines = from_everyone(line.reshape(1, -1), VOCAB).reshape(-1, line.size)

    def joined(logs):
        peak = jnp.max(logs, axis=0)
        return peak + jnp.log(jnp.sum(jnp.exp(logs - peak), axis=0))

    log_b = joined(lines[:, :tokens])
    log_a = joined(lines[:, tokens : 2 * tokens])
    label_a = jnp.sum(lines[:, 2 * tokens : 3 * tokens], axis=0)
    loss_a = log_a - label_a
    amax_scale = (448.0 / jnp.max(lines[:, 3 * tokens :])).reshape(1).astype(jnp.float32)

    onehot = (column == labels_b[:, None]).astype(jnp.float32)
    dlogits_b = ((jnp.exp(scores_b - log_b[:, None]) - onehot) * loss_cotangent[:, None]).astype(
        jnp.bfloat16
    )

    def grad_rows(flip):
        return lax.dot_general(
            weights[flip], dlogits_b, (((1,), (1,)), ((), ())), preferred_element_type=jnp.float32
        )

    dlogits_b = lax.optimization_barrier(dlogits_b)
    total = lax.optimization_barrier(grad_rows((0, 0)))
    for flip in FLIPS:
        total = total + exchanged(grad_rows(flip).astype(jnp.bfloat16), flip).astype(jnp.float32)
    parts = total.astype(jnp.bfloat16).reshape(lattice, width, tokens)
    parts = lax.all_to_all(parts, LATTICE, 0, 0, tiled=True)
    grad_hidden_b = jnp.sum(parts.astype(jnp.float32), axis=0).astype(jnp.bfloat16).T
    return (scores_a.astype(jnp.bfloat16), loss_a, amax_scale, grad_hidden_b)


def solution(mesh):
    finer = Mesh(mesh.devices.reshape(4, 2, 4, 2, mesh.shape["pipe"]), (*VOCAB, "pipe"))
    placed = (P("pipe", VOCAB), P("pipe"), P("pipe", VOCAB), P("pipe"), P("pipe"), P("pipe", VOCAB))

    return jax.shard_map(
        shards,
        mesh=finer,
        in_specs=placed,
        out_specs=(P("pipe", VOCAB), P("pipe"), P("pipe"), P("pipe", VOCAB)),
        check_vma=False,
    )
```

```python
import jax
import jax.numpy as jnp
from jax import lax
from jax.sharding import Mesh
from jax.sharding import PartitionSpec as P


Z, Y = ("z_two", "z_one"), ("y_two", "y_one")
VOCAB = (*Z, *Y)
LATTICE, QUAD = ("z_two", "y_two"), ("z_one", "y_one")
FLIPS = ((1, 1), (1, 0), (0, 1))


def size(axes):
    return lax.axis_size(axes)


def from_everyone(x, axes):
    return lax.all_to_all(jnp.broadcast_to(x[None], (size(axes), *x.shape)), axes, 0, 0, tiled=True)


def neighbour(i, n, shift):
    return (i + 1 - 2 * ((i + shift) % 2) + n) % n


def exchanged(x, flip):
    shift = flip[0] * flip[1]
    nz, ny = size(Z), size(Y)
    pairs = []
    for z in range(nz):
        for y in range(ny):
            there = neighbour(z, nz, shift) if flip[0] else z, neighbour(y, ny, shift) if flip[1] else y
            pairs.append((z * ny + y, there[0] * ny + there[1]))
    return lax.ppermute(x, VOCAB, pairs)


def shards(hidden_a, labels_a, hidden_b, labels_b, loss_cotangent, out_weight):
    tokens, width = hidden_a.shape
    columns = out_weight.shape[1]
    offset = lax.axis_index(VOCAB) * columns
    lattice = size(LATTICE)
    half = lattice * width // 2
    by_class = out_weight.reshape(size(Z[0]), 2, size(Y[0]), 2, width, columns)

    def weight_rows(flip):
        z, y = lax.axis_index(Z[1]), lax.axis_index(Y[1])
        at = (0, z + flip[0] - 2 * z * flip[0], 0, y + flip[1] - 2 * y * flip[1], 0, 0)
        counts = (by_class.shape[0], 1, by_class.shape[2], 1, width, columns)
        return lax.dynamic_slice(by_class, at, counts).reshape(2 * half, columns)

    weights = {flip: weight_rows(flip) for flip in ((0, 0), *FLIPS)}

    def product(block, rows):
        return lax.dot_general(
            block, rows, (((0,), (0,)), ((), ())), preferred_element_type=jnp.float32
        )

    own = jnp.concatenate([hidden_b.T, hidden_a.T], axis=1)
    mine = from_everyone(own, LATTICE).reshape(2 * half, 2 * tokens)

    def scores_of(mine):
        scores = product(mine, weights[0, 0])
        for flip in FLIPS:
            block = exchanged(mine, flip)
            scores = scores + product(block, weights[flip])
        return scores

    scores_b = scores_of(mine[:, :tokens])
    scores_a = scores_of(mine[:, tokens:])
    column = offset + lax.broadcasted_iota(jnp.int32, (1, columns), 1)
    column_a = lax.optimization_barrier(column)

    def log_total(scores):
        peak = jnp.max(scores, axis=1)
        return peak + jnp.log(jnp.sum(jnp.exp(scores - peak[:, None]), axis=1))

    def joined(logs):
        peak = jnp.max(logs, axis=0)
        return peak + jnp.log(jnp.sum(jnp.exp(logs - peak), axis=0))

    log_b = joined(from_everyone(log_total(scores_b).reshape(1, -1), VOCAB).reshape(-1, tokens))
    label_own = jnp.sum(jnp.where(column_a == labels_a[:, None], scores_a, 0.0), axis=1)
    largest = jnp.broadcast_to(jnp.max(jnp.abs(scores_a)), (tokens,))
    lines = jnp.stack([log_total(scores_a), label_own, largest])

    def joined_lines(lines):
        return jnp.stack(
            [joined(lines[:, 0]), jnp.sum(lines[:, 1], axis=0), jnp.max(lines[:, 2], axis=0)]
        )

    quad = joined_lines(from_everyone(lines, QUAD).reshape(-1, *lines.shape))
    high = lax.reduce_precision(quad, 8, 7)
    riders = jnp.concatenate([high, quad - high, jnp.zeros_like(quad[:2])]).astype(jnp.bfloat16)

    onehot = (column == labels_b[:, None]).astype(jnp.float32)
    dlogits_b = ((jnp.exp(scores_b - log_b[:, None]) - onehot) * loss_cotangent[:, None]).astype(
        jnp.bfloat16
    )

    dlogits_b = lax.optimization_barrier(dlogits_b)

    def grad_rows(flip):
        return lax.dot_general(
            weights[flip], dlogits_b, (((1,), (1,)), ((), ())), preferred_element_type=jnp.float32
        )

    total = lax.optimization_barrier(grad_rows((0, 0)))
    for flip in FLIPS:
        total = total + exchanged(grad_rows(flip).astype(jnp.bfloat16), flip).astype(jnp.float32)
    parts = total.astype(jnp.bfloat16).reshape(lattice, width, tokens)
    parts = jnp.concatenate([parts, jnp.broadcast_to(riders[None], (lattice, *riders.shape))], axis=1)
    parts = lax.all_to_all(parts, LATTICE, 0, 0, tiled=True)
    grad_hidden_b = jnp.sum(parts[:, :width].astype(jnp.float32), axis=0).astype(jnp.bfloat16).T
    came = parts[:, width : width + 6].astype(jnp.float32)
    log_a, label_a, largest = joined_lines(came[:, :3] + came[:, 3:])
    loss_a = log_a - label_a
    amax_scale = (448.0 / largest[:1]).astype(jnp.float32)
    return (scores_a.astype(jnp.bfloat16), loss_a, amax_scale, grad_hidden_b)


def solution(mesh):
    finer = Mesh(mesh.devices.reshape(4, 2, 4, 2, mesh.shape["pipe"]), (*VOCAB, "pipe"))
    placed = (P("pipe", VOCAB), P("pipe"), P("pipe", VOCAB), P("pipe"), P("pipe"), P("pipe", VOCAB))

    return jax.shard_map(
        shards,
        mesh=finer,
        in_specs=placed,
        out_specs=(P("pipe", VOCAB), P("pipe"), P("pipe"), P("pipe", VOCAB)),
        check_vma=False,
    )
```

```python
import jax
import jax.numpy as jnp
from jax import lax
from jax.sharding import Mesh
from jax.sharding import PartitionSpec as P


Z, Y = ("z_two", "z_one"), ("y_two", "y_one")
VOCAB = (*Z, *Y)
LATTICE, QUAD = ("z_two", "y_two"), ("z_one", "y_one")
FLIPS = ((1, 1), (1, 0), (0, 1))


def size(axes):
    return lax.axis_size(axes)


def from_everyone(x, axes):
    return lax.all_to_all(jnp.broadcast_to(x[None], (size(axes), *x.shape)), axes, 0, 0, tiled=True)


def neighbour(i, n, shift):
    return (i + 1 - 2 * ((i + shift) % 2) + n) % n


def exchanged(x, flip):
    shift = flip[0] * flip[1]
    nz, ny = size(Z), size(Y)
    pairs = []
    for z in range(nz):
        for y in range(ny):
            there = neighbour(z, nz, shift) if flip[0] else z, neighbour(y, ny, shift) if flip[1] else y
            pairs.append((z * ny + y, there[0] * ny + there[1]))
    return lax.ppermute(x, VOCAB, pairs)


def shards(hidden_a, labels_a, hidden_b, labels_b, loss_cotangent, out_weight):
    tokens, width = hidden_a.shape
    columns = out_weight.shape[1]
    offset = lax.axis_index(VOCAB) * columns
    lattice = size(LATTICE)
    half = lattice * width // 2
    by_class = out_weight.reshape(size(Z[0]), 2, size(Y[0]), 2, width, columns)

    def weight_rows(flip):
        z, y = lax.axis_index(Z[1]), lax.axis_index(Y[1])
        at = (0, z + flip[0] - 2 * z * flip[0], 0, y + flip[1] - 2 * y * flip[1], 0, 0)
        counts = (by_class.shape[0], 1, by_class.shape[2], 1, width, columns)
        return lax.dynamic_slice(by_class, at, counts).reshape(2 * half, columns)

    weights = {flip: weight_rows(flip) for flip in ((0, 0), *FLIPS)}

    def product(block, rows):
        return lax.dot_general(
            block, rows, (((0,), (0,)), ((), ())), preferred_element_type=jnp.float32
        )

    own = jnp.concatenate([hidden_b.T, hidden_a.T], axis=1)
    mine = from_everyone(own, LATTICE).reshape(2 * half, 2 * tokens)

    def scores_of(mine):
        scores = product(mine, weights[0, 0])
        for flip in FLIPS:
            block = exchanged(mine, flip)
            scores = lax.optimization_barrier(scores) + product(block, weights[flip])
        return scores

    scores_b = scores_of(lax.optimization_barrier(mine[:, :tokens]))
    scores_a = scores_of(mine[:, tokens:])
    column = offset + lax.broadcasted_iota(jnp.int32, (1, columns), 1)
    column_a = lax.optimization_barrier(column)

    def log_total(scores):
        peak = jnp.max(scores, axis=1)
        return peak + jnp.log(jnp.sum(jnp.exp(scores - peak[:, None]), axis=1))

    def joined(logs):
        peak = jnp.max(logs, axis=0)
        return peak + jnp.log(jnp.sum(jnp.exp(logs - peak), axis=0))

    log_b = joined(from_everyone(log_total(scores_b).reshape(1, -1), VOCAB).reshape(-1, tokens))
    label_own = jnp.sum(jnp.where(column_a == labels_a[:, None], scores_a, 0.0), axis=1)
    largest = jnp.broadcast_to(jnp.max(jnp.abs(scores_a)), (tokens,))
    lines = jnp.stack([log_total(scores_a), label_own, largest])

    def joined_lines(lines):
        return jnp.stack(
            [joined(lines[:, 0]), jnp.sum(lines[:, 1], axis=0), jnp.max(lines[:, 2], axis=0)]
        )

    quad = joined_lines(from_everyone(lines, QUAD).reshape(-1, *lines.shape))
    high = lax.reduce_precision(quad, 8, 7)
    riders = jnp.concatenate([high, quad - high, high[:2]]).astype(jnp.bfloat16)

    onehot = (column == labels_b[:, None]).astype(jnp.float32)
    dlogits_b = ((jnp.exp(scores_b - log_b[:, None]) - onehot) * loss_cotangent[:, None]).astype(
        jnp.bfloat16
    )

    dlogits_b = lax.optimization_barrier(dlogits_b)

    def grad_rows(flip):
        return lax.dot_general(
            weights[flip], dlogits_b, (((1,), (1,)), ((), ())), preferred_element_type=jnp.float32
        )

    total = lax.optimization_barrier(grad_rows((0, 0)))
    for flip in FLIPS:
        total = total + exchanged(grad_rows(flip).astype(jnp.bfloat16), flip).astype(jnp.float32)
    parts = total.astype(jnp.bfloat16).reshape(lattice, width, tokens)
    parts = jnp.concatenate([parts, jnp.broadcast_to(riders[None], (lattice, *riders.shape))], axis=1)
    parts = lax.all_to_all(parts, LATTICE, 0, 0, tiled=True)
    grad_hidden_b = jnp.sum(parts[:, :width].astype(jnp.float32), axis=0).astype(jnp.bfloat16).T
    came = parts[:, width : width + 6].astype(jnp.float32)
    log_a, label_a, largest = joined_lines(came[:, :3] + came[:, 3:])
    loss_a = log_a - label_a
    amax_scale = (448.0 / largest[:1]).astype(jnp.float32)
    return (scores_a.astype(jnp.bfloat16), loss_a, amax_scale, grad_hidden_b)


def solution(mesh):
    finer = Mesh(mesh.devices.reshape(4, 2, 4, 2, mesh.shape["pipe"]), (*VOCAB, "pipe"))
    placed = (P("pipe", VOCAB), P("pipe"), P("pipe", VOCAB), P("pipe"), P("pipe"), P("pipe", VOCAB))

    return jax.shard_map(
        shards,
        mesh=finer,
        in_specs=placed,
        out_specs=(P("pipe", VOCAB), P("pipe"), P("pipe"), P("pipe", VOCAB)),
        check_vma=False,
    )
```
